128 devices in a mesh: stn: 16 (over y_lo, z, core), chan: 8 (over y_hi, x).
Axes of the slice: x: 4, y: 4 (y_hi: 2, y_lo: 2; y = y_hi * 2 + y_lo), z: 4, core: 2. Of those that a mesh axis runs over, the one named last changes fastest.
Arguments:
- voltages: bfloat16 [16, 2, 256, 131072], P('stn', None, None, 'chan'), may hold values from -6 to 6
- positions: float32 [16, 3, 256], P('stn'), may hold values from -4 to 4
- directions: float32 [3, 64], replicated, may hold values from -0.5 to 0.5
- flag_mask: int32 [16, 2, 2048], P('stn', None, 'chan'), may hold values from 0 to 1, as said below
- tapers: float32 [16, 8], P('stn'), may hold values from 0.3 to 3
- weight_index: int32 [16, 64], P('stn'), may hold values from 0 to 7
Outputs:
- beam_power: float32 [64, 131072], P('stn', 'chan')
- beam_total: float32 [64], P('stn')
The draws below stay inside these ranges and needn't reach their ends.
Inputs may be any that keep to these rules, and one draw needn't show every extreme that they name: `flag_mask`: the first block of station 0 is kept in every channel.
All inputs are finite; a program needn't handle non-finite values.
Results may differ from the reference program's by a relative error of at most 0.003.
Values sent between devices are 32-bit elements; how exact they have to be, the bound alone decides.
No kernel may reach another device: no remote copies, remote signals or barrier semaphores. Data moves between devices by JAX's collectives and lax.ppermute only.
A program may use at most 192 MiB of HBM per device.

```python
import math
import jax
import jax.numpy as jnp
from jax import lax

DIPOLES = 256
BLOCK = 128
DBLOCKS = 2
BEAMS = 64
CHANNELS = 2048
SAMPLES = 64
STATIONS = 16
TAPERS = 8


def draw_flag_mask(key, part):
    levels = jax.random.randint(key, (STATIONS, DBLOCKS, CHANNELS), 0, 4)
    kept = (levels > 0).astype(jnp.int32)
    station_ids = lax_free_iota_station()
    return jnp.where(station_ids, jnp.int32(1), kept)


def lax_free_iota_station():
    station_ids = jnp.arange(STATIONS).astype(jnp.int32)[:, None, None]
    block_ids = jnp.arange(DBLOCKS).astype(jnp.int32)[None, :, None]
    first = (station_ids == 0) & (block_ids == 0)
    return jnp.broadcast_to(first, (STATIONS, DBLOCKS, CHANNELS))


def place_ends(values, stream_key, least, high):
    shape = values.shape
    index_at = [jax.random.randint(jax.random.fold_in(stream_key, axis), (), 0, shape[axis]) for axis in range(len(shape))]
    values = values.at[tuple(index_at)].set(least)
    longest = shape.index(max(shape))
    index_at[longest] = (index_at[longest] + 1) % shape[longest]
    return values.at[tuple(index_at)].set(high)


def shard_levels(own_key, extent, pieces, low, high):
    factor_of = 1.0
    for position, shards_of in pieces:
        heights = jax.random.uniform(jax.random.fold_in(jax.random.fold_in(own_key, 6), position), (shards_of,), jnp.float32, low / len(pieces), high / len(pieces))
        factor_of = factor_of * jnp.repeat(jnp.exp(heights), extent[position] // shards_of).reshape((-1,) + (1,) * (len(extent) - 1 - position))
    return factor_of


def scatter_about(rng, shape, scale, most, shards=(), kind=jnp.bfloat16):
    level = shard_levels(rng, shape, shards, -0.22, 0.18) if shards else 1.0
    drawn = jax.random.normal(rng, shape, jnp.float32) * scale * level
    return jnp.minimum(jnp.maximum(drawn, -most), most).astype(kind)


def setup_inputs(seed: int = 0) -> dict:
    arg_keys = jax.random.split(jax.random.key(seed), 7)
    voltages = scatter_about(arg_keys[0], (STATIONS, 2, DIPOLES, CHANNELS * SAMPLES), 1.0, 6.0, ((0, 16), (3, 8)))
    positions = jnp.clip(jax.random.uniform(arg_keys[1], (STATIONS, 3, DIPOLES), jnp.float32, -4.0, 4.0) * shard_levels(arg_keys[1], (STATIONS, 3, DIPOLES), ((0, 16),), -0.4, 0.0), -4.0, 4.0)
    directions = jnp.clip(jax.random.uniform(arg_keys[2], (3, BEAMS), jnp.float32, -0.5, 0.5), -0.5, 0.5)
    flag_mask = draw_flag_mask(jax.random.fold_in(arg_keys[6], 71), 0)
    tapers = jnp.clip(jnp.exp(math.log(3.0) - 2.3025851 * jax.random.uniform(arg_keys[4], (STATIONS, TAPERS), jnp.float32) ** shard_levels(arg_keys[4], (STATIONS, TAPERS), ((0, 16),), -0.2, 0.2)), 0.3, 3.0)
    weight_index = place_ends(jax.random.randint(arg_keys[5], (STATIONS, BEAMS), 0, TAPERS), jax.random.fold_in(arg_keys[5], 1), 0, TAPERS - 1).astype(jnp.int32)
    return dict(voltages=voltages, positions=positions, directions=directions, flag_mask=flag_mask, tapers=tapers, weight_index=weight_index)


def station_beam(volts, place, keep_flags, weight_row, directions, ratio):
    delay = directions[0][:, None] * place[0][None, :] + directions[1][:, None] * place[1][None, :] + directions[2][:, None] * place[2][None, :]
    phase = (2.0 * math.pi) * delay[:, :, None] * ratio[None, None, :]
    blocks = keep_flags.shape[0]
    keep = jnp.broadcast_to(keep_flags.astype(jnp.float32)[:, None, :], (blocks, BLOCK, keep_flags.shape[1])).reshape(blocks * BLOCK, keep_flags.shape[1])
    amplitude = weight_row[:, None, None] * keep[None, :, :]
    steer_real = (amplitude * jnp.cos(phase)).astype(jnp.bfloat16).astype(jnp.float32)
    steer_imag = (-amplitude * jnp.sin(phase)).astype(jnp.bfloat16).astype(jnp.float32)
    signal = volts.astype(jnp.float32).reshape(2, volts.shape[1], keep_flags.shape[1], -1)
    high = lax.Precision.HIGHEST
    real_part = jnp.einsum('bdc,dct->bct', steer_real, signal[0], precision=high) - jnp.einsum('bdc,dct->bct', steer_imag, signal[1], precision=high)
    imag_part = jnp.einsum('bdc,dct->bct', steer_real, signal[1], precision=high) + jnp.einsum('bdc,dct->bct', steer_imag, signal[0], precision=high)
    return jnp.stack((real_part, imag_part), axis=0)


def reference(voltages, positions, directions, flag_mask, tapers, weight_index):
    ratio = 1.0 + 0.5 * jnp.arange(CHANNELS).astype(jnp.float32) / CHANNELS
    choose = (weight_index[:, :, None] == jnp.arange(TAPERS).astype(jnp.int32)[None, None, :]).astype(jnp.float32)
    station_weight = jnp.sum(choose * tapers[:, None, :], axis=2)
    alive = jnp.sum(flag_mask, axis=1).astype(jnp.float32) * BLOCK
    counts = jnp.dot(station_weight.T, alive, precision=lax.Precision.HIGHEST)

    def add_station(total, items):
        volts, place, keep_flags, weight_row = items
        return total + station_beam(volts, place, keep_flags, weight_row, directions, ratio), None

    start = jnp.zeros((2, BEAMS, CHANNELS, SAMPLES), jnp.float32)
    partial_value, unused = lax.scan(add_station, start, (voltages, positions, flag_mask, station_weight))
    scaled = partial_value / counts[None, :, :, None]
    power = scaled[0] * scaled[0] + scaled[1] * scaled[1]
    beam_power = power.reshape(BEAMS, CHANNELS * SAMPLES)
    beam_total = jnp.sum(beam_power, axis=1)
    return beam_power, beam_total
```

```python
import jax
import jax.numpy as jnp
from jax import lax
from jax.experimental import pallas as pl
from jax.experimental.pallas import tpu as pltpu
from jax.sharding import PartitionSpec as P

BLOCK = 128
GROUP = 16
PAD = 128
Y, Z, CORE = 2, 4, 2
PIECES = (1, 1, 1, 1)

def poly(coefs, x):
    total = jnp.full(x.shape, coefs[-1], jnp.float32)
    for c in coefs[-2::-1]:
        total = total * x + c
    return total


def turn(r, terms):
    x = r * r
    return poly(COS7[: terms], x), r * poly(SIN7[: terms], x)


SIN7 = (
    6.283185307136744,
    -41.34170221839102,
    81.60524742222256,
    -76.70580022497265,
    42.057754062457725,
    -15.086565424172946,
    3.781319130391277,
    -0.6207787856421599,
)
COS7 = (
    0.9999999998857545,
    -19.73920874347965,
    64.93938907682282,
    -85.4566583290415,
    60.24213144377024,
    -26.404668561864113,
    7.800131962320425,
    -1.4531123696403512,
)
SINT = (6.283185307179586, -41.34170224039975, 81.60524927607504)
COST = (1.0, -19.739208802178716, 64.93939402266829, -85.45681720669373)


def beam_kernel(
    pos_ref, dir_ref, tap_ref, index_ref, flag_ref, flagv_ref, volt_ref, send_ref, keep_ref,
    buf, sems, t_ref, u_ref, fr_ref, fi_ref, *, start, count, whole,
):
    width = 64 * GROUP
    groups = count // GROUP

    def fetch(g):
        return pltpu.make_async_copy(
            volt_ref.at[0, :, :, pl.ds((start + g * GROUP) * 64, width)],
            buf.at[:, :, pl.ds(g * width, width)],
            sems.at[g],
        )

    for g in range(groups):
        fetch(g).start()

    me = lax.axis_index("stn")
    my_core = me % CORE
    my_z = (me // CORE) % Z
    my_y = me // (CORE * Z)
    rows = lax.broadcasted_iota(jnp.int32, (128, 64), 0)
    tile, sub = rows // 8, rows % 8
    core = jnp.where(tile // 8 == 1, my_core, 1 - my_core)
    y = jnp.where((tile // 4) % 2 == 1, my_y, 1 - my_y)
    order = tile % 4
    shift = jnp.where(order == 0, 2, jnp.where(order == 1, 1, jnp.where(order == 2, 3, 0)))
    z = (my_z + shift) % Z
    beam = y * 32 + z * 8 + core * 4 + sub % 4
    chosen = beam == lax.broadcasted_iota(jnp.int32, (128, 64), 1)

    def column(row):
        return jnp.sum(jnp.where(chosen, row, 0.0), axis=1, keepdims=True)

    weight_row = jnp.zeros((1, 64), jnp.float32)
    for e in range(tap_ref.shape[1]):
        weight_row = weight_row + jnp.where(index_ref[...] == e, tap_ref[0, e], 0.0)
    weight = column(weight_row)
    delay = (
        column(dir_ref[0:1, :]) * pos_ref[0, 0:1, :]
        + column(dir_ref[1:2, :]) * pos_ref[0, 1:2, :]
        + column(dir_ref[2:3, :]) * pos_ref[0, 2:3, :]
    )
    first = lax.axis_index("chan") * (whole // lax.axis_size("chan")) + start
    ratio = 1.0 + 0.5 * (first.astype(jnp.float32) / whole)
    turns = delay * ratio
    cos, sin = turn(turns - jnp.round(turns), 8)
    real = lax.broadcasted_iota(jnp.int32, (128, 256), 0) % 8 < 4
    t_ref[...] = weight * jnp.where(real, cos, -sin)
    u_ref[...] = weight * jnp.where(real, sin, cos)
    step = delay * (0.5 / whole)
    for j in range(GROUP + 1):
        r = step * float(j)
        x = r * r
        fr_ref[j] = poly(COST, x)
        fi_ref[j] = -(r * poly(SINT, x))

    alive = (flagv_ref[0, 0:1, :] + flagv_ref[0, 1:2, :]).astype(jnp.float32) * float(BLOCK)
    lanes = (start // 128) * 128
    share = weight[:, :] * alive[:, lanes : lanes + 128]
    send_ref[:, pl.ds(count * 64, PAD)] = share[:64]
    keep_ref[:, pl.ds(count * 64, PAD)] = share[64:]

    left = lax.broadcasted_iota(jnp.int32, (128, 128), 1) < 64
    sign = jnp.where(lax.broadcasted_iota(jnp.int32, (128, 128), 0) % 8 < 4, -1.0, 1.0)

    def group(g, carry):
        fetch(g).wait()
        t = t_ref[...]
        u = u_ref[...]

        def steer(j):
            value = (t * fr_ref[j] + u * fi_ref[j]).astype(jnp.bfloat16)
            at = start + g * GROUP + j
            halves = []
            for k in range(2):
                keep = flag_ref[0, k, at].astype(jnp.float32)
                keep = jnp.full((128, 128), keep, jnp.float32).astype(jnp.bfloat16)
                halves.append(value[:, 128 * k : 128 * k + 128] * keep)
            return jnp.concatenate(halves, axis=1)

        for p in range(GROUP // 2):
            lhs = jnp.concatenate((steer(2 * p), steer(2 * p + 1)), axis=0)
            at = pl.multiple_of(g * width + p * 128, 128)
            rhs = jnp.concatenate((buf[0, :, pl.ds(at, 128)], buf[1, :, pl.ds(at, 128)]), axis=1)
            both = jnp.dot(lhs, rhs, preferred_element_type=jnp.float32)
            by_real = jnp.where(left, both[:128, :128], both[128:, :128])
            by_imag = jnp.where(left, both[:128, 128:], both[128:, 128:])
            swapped = pltpu.roll(by_imag.reshape(16, 8, 128), 4, 1).reshape(128, 128)
            out = by_real + swapped * sign
            send_ref[:, pl.ds(at, 128)] = out[:64]
            keep_ref[:, pl.ds(at, 128)] = out[64:]
        t_ref[...] = t * fr_ref[GROUP] + u * fi_ref[GROUP]
        u_ref[...] = u * fr_ref[GROUP] - t * fi_ref[GROUP]
        return carry

    lax.fori_loop(0, groups, group, 0)


def core_kernel(keep_ref, got_ref, up_ref, down_ref, rest_ref):
    def block(i):
        return keep_ref[8 * i : 8 * i + 8] + got_ref[8 * i : 8 * i + 8]

    up_ref[0:8] = block(0)
    up_ref[8:16] = block(5)
    down_ref[0:8] = block(4)
    down_ref[8:16] = block(2)
    rest_ref[0:8] = block(1)
    rest_ref[8:16] = block(6)
    rest_ref[16:24] = block(3)
    rest_ref[24:32] = block(7)


def merge_kernel(rest_ref, up_ref, down_ref, up2_ref, down2_ref, own_ref):
    up2_ref[...] = rest_ref[0:8] + up_ref[0:8]
    down2_ref[...] = rest_ref[8:16] + down_ref[0:8]
    own_ref[0:8] = rest_ref[16:24] + down_ref[8:16]
    own_ref[8:16] = rest_ref[24:32] + up_ref[8:16]


def z_kernel(own_ref, up2_ref, down2_ref, send_ref, mine_ref):
    send_ref[...] = own_ref[0:8] + up2_ref[...]
    mine_ref[...] = own_ref[8:16] + down2_ref[...]


def final_kernel(*refs, spans):
    pieces = len(spans)
    mine, got = refs[:pieces], refs[pieces : 2 * pieces]
    power_ref, total_ref = refs[2 * pieces :]
    left = lax.broadcasted_iota(jnp.int32, (8, 128), 1) < 64
    total = jnp.zeros((8, 128), jnp.float32)
    for piece, (start, count) in enumerate(spans):
        counts = mine[piece][:, pl.ds(count * 64, PAD)] + got[piece][:, pl.ds(count * 64, PAD)]
        counts = jnp.where(lax.broadcasted_iota(jnp.int32, (8, 128), 0) < 4, counts, 1.0)
        inside = lax.broadcasted_iota(jnp.int32, (8, 128), 1)
        begin = start % 128
        inside = (inside >= begin) & (inside < begin + count)
        inverse = 1.0 / jnp.where(inside, counts, 1.0)
        for p in range(count // 2):
            value = mine[piece][:, pl.ds(p * 128, 128)] + got[piece][:, pl.ds(p * 128, 128)]
            square = value * value
            square = square + pltpu.roll(square, 4, 0)
            c = begin + 2 * p
            scale = jnp.where(left, inverse[:, c : c + 1], inverse[:, c + 1 : c + 2])
            power = square * (scale * scale)
            power_ref[:, pl.ds(start * 64 + p * 128, 128)] = power[:4]
            total = total + power
    total_ref[...] = jnp.broadcast_to(jnp.sum(total, axis=1, keepdims=True), (8, 128))


def vmem(n):
    return [pl.BlockSpec(memory_space=pltpu.VMEM)] * n


def on_device(voltages, positions, directions, flag_mask, tapers, weight_index):
    chan_local = flag_mask.shape[2]
    whole = chan_local * lax.axis_size("chan")
    unit = chan_local // sum(PIECES)
    spans = []
    for size in PIECES:
        spans.append((sum(s[1] for s in spans), size * unit))

    def number(y, z, core):
        return y * Z * CORE + z % Z * CORE + core

    def pairs(to):
        return [
            (number(y, z, c), number(*to(y, z, c)))
            for y in range(Y) for z in range(Z) for c in range(CORE)
        ]

    to_core = pairs(lambda y, z, c: (y, z, 1 - c))
    to_up = pairs(lambda y, z, c: (y, z + 1, c))
    to_down = pairs(lambda y, z, c: (y, z - 1, c))
    to_y = pairs(lambda y, z, c: (1 - y, z, c))

    def shaped(rows, lanes):
        return jax.ShapeDtypeStruct((rows, lanes), jnp.float32)

    mines, gots = [], []
    for start, count in spans:
        lanes = count * 64 + PAD
        send, keep = pl.pallas_call(
            lambda *refs, start=start, count=count: beam_kernel(
                *refs, start=start, count=count, whole=whole
            ),
            out_shape=(shaped(64, lanes), shaped(64, lanes)),
            in_specs=vmem(2)
            + [pl.BlockSpec(memory_space=pltpu.SMEM)]
            + vmem(1)
            + [pl.BlockSpec(memory_space=pltpu.SMEM)]
            + vmem(1)
            + [pl.BlockSpec(memory_space=pl.ANY)],
            out_specs=tuple(vmem(2)),
            scratch_shapes=[
                pltpu.VMEM((2, 256, count * 64), jnp.bfloat16),
                pltpu.SemaphoreType.DMA((count // GROUP,)),
                pltpu.VMEM((128, 256), jnp.float32),
                pltpu.VMEM((128, 256), jnp.float32),
                pltpu.VMEM((GROUP + 1, 128, 256), jnp.float32),
                pltpu.VMEM((GROUP + 1, 128, 256), jnp.float32),
            ],
            compiler_params=pltpu.CompilerParams(vmem_limit_bytes=24 * 2**20),
            name="beam",
        )(positions, directions, tapers, weight_index, flag_mask, flag_mask, voltages)
        got = lax.ppermute(send, "stn", to_core)
        up, down, rest = pl.pallas_call(
            core_kernel,
            out_shape=(shaped(16, lanes), shaped(16, lanes), shaped(32, lanes)),
            in_specs=vmem(2), out_specs=tuple(vmem(3)), name="core_sum",
        )(keep, got)
        up = lax.ppermute(up, "stn", to_up)
        down = lax.ppermute(down, "stn", to_down)
        up2, down2, own = pl.pallas_call(
            merge_kernel,
            out_shape=(shaped(8, lanes), shaped(8, lanes), shaped(16, lanes)),
            in_specs=vmem(3), out_specs=tuple(vmem(3)), name="merge",
        )(rest, up, down)
        up2 = lax.ppermute(up2, "stn", to_up)
        down2 = lax.ppermute(down2, "stn", to_down)
        over, mine = pl.pallas_call(
            z_kernel,
            out_shape=(shaped(8, lanes), shaped(8, lanes)),
            in_specs=vmem(3), out_specs=tuple(vmem(2)), name="z_sum",
        )(own, up2, down2)
        mines.append(mine)
        gots.append(lax.ppermute(over, "stn", to_y))

    beam_power, total = pl.pallas_call(
        lambda *refs: final_kernel(*refs, spans=spans),
        out_shape=(shaped(4, chan_local * 64), shaped(8, 128)),
        in_specs=vmem(2 * len(spans)), out_specs=tuple(vmem(2)), name="power",
    )(*mines, *gots)
    n = lax.axis_size("chan")
    total = total[:, 0]
    for flip in (1, 3, 4):
        total = total + lax.ppermute(total, "chan", [(i, i ^ flip) for i in range(n)])
    return (beam_power, total[:4])


def solution(mesh):
    in_specs = (
        P("stn", None, None, "chan"),
        P("stn", None, None),
        P(),
        P("stn", None, "chan"),
        P("stn", None),
        P("stn", None),
    )
    out_specs = (P("stn", "chan"), P("stn"))
    return jax.shard_map(
        on_device, mesh=mesh, in_specs=in_specs, out_specs=out_specs, check_vma=False
    )
```

```python
import jax
import jax.numpy as jnp
from jax import lax
from jax.experimental import pallas as pl
from jax.experimental.pallas import tpu as pltpu
from jax.sharding import PartitionSpec as P


BLOCK = 128
GROUP = 16
HALF = GROUP // 2
PAD = 128
Y, Z, CORE = 2, 4, 2
CHUNKS = ((3, "aby"), (4, "bya"), (4, "yab"), (3, "aby"), (2, "bya"))

SIN = (
    6.283185307136744,
    -41.34170221839102,
    81.60524742222256,
    -76.70580022497265,
    42.057754062457725,
    -15.086565424172946,
    3.781319130391277,
    -0.6207787856421599,
)
COS = (
    0.9999999998857545,
    -19.73920874347965,
    64.93938907682282,
    -85.4566583290415,
    60.24213144377024,
    -26.404668561864113,
    7.800131962320425,
    -1.4531123696403512,
)
SIN_NEAR = (6.283185307179586, -41.34170224039975, 81.60524927607504)
COS_NEAR = (1.0, -19.739208802178716, 64.93939402266829, -85.45681720669373)


def poly(coefs, x):
    total = jnp.full(x.shape, coefs[-1], jnp.float32)
    for c in coefs[-2::-1]:
        total = total * x + c
    return total


def places(order):
    out = []
    for tile in range(16):
        moved = {"y": (tile // 4) % 2, "b": (tile // 2) % 2, "a": tile % 2}
        at = sum((1 - moved[name]) << (2 - i) for i, name in enumerate(order))
        out.append((tile // 8, at))
    return out


def make_tables(
    pos_ref, dir_ref, tap_ref, index_ref,
    t_ref, u_ref, fr_ref, fi_ref, mask_ref, share_ref, sums_ref, whole,
):
    me = lax.axis_index("stn")
    my_core = me % CORE
    my_z = (me // CORE) % Z
    my_y = me // (CORE * Z)
    rows = lax.broadcasted_iota(jnp.int32, (128, 64), 0)
    tile, sub = rows // 8, rows % 8
    core = jnp.where(tile // 8 == 1, my_core, 1 - my_core)
    y = jnp.bitwise_xor((tile // 4) % 2, my_y)
    z = jnp.bitwise_xor(jnp.bitwise_xor(tile % 2, 3 * ((tile // 2) % 2)), my_z)
    beam = y * (64 // Y) + z * (64 // (Y * Z)) + core * 4 + sub % 4
    chosen = beam == lax.broadcasted_iota(jnp.int32, (128, 64), 1)

    def column(row):
        return jnp.sum(jnp.where(chosen, row, 0.0), axis=1, keepdims=True)

    weight_row = jnp.zeros((1, 64), jnp.float32)
    for e in range(tap_ref.shape[1]):
        weight_row = weight_row + jnp.where(index_ref[...] == e, tap_ref[0, e], 0.0)
    weight = column(weight_row)
    delay = (
        column(dir_ref[0:1, :]) * pos_ref[0]
        + column(dir_ref[1:2, :]) * pos_ref[1]
        + column(dir_ref[2:3, :]) * pos_ref[2]
    )
    channel = lax.axis_index("chan") * (whole // lax.axis_size("chan"))
    ratio = 1.0 + 0.5 * ((channel.astype(jnp.float32) + (HALF - 0.5)) / whole)
    turns = delay * ratio
    r = turns - jnp.round(turns)
    x = r * r
    cos, sin = poly(COS, x), r * poly(SIN, x)
    real = lax.broadcasted_iota(jnp.int32, (128, 256), 0) % 8 < 4
    t_ref[...] = weight * jnp.where(real, cos, -sin)
    u_ref[...] = weight * jnp.where(real, sin, cos)
    step = delay * (0.5 / whole)

    def factor(r):
        x = r * r
        return poly(COS_NEAR, x), -(r * poly(SIN_NEAR, x))

    def times(v, w):
        return v[0] * w[0] - v[1] * w[1], v[0] * w[1] + v[1] * w[0]

    half = factor(0.5 * step)
    one = factor(step)
    for j in range(HALF):
        fr_ref[j], fi_ref[j] = half
        last, half = half, times(half, one)
    fr_ref[HALF], fi_ref[HALF] = times(half, last)
    alive = (sums_ref[0, 0:1, :] + sums_ref[0, 1:2, :]).astype(jnp.float32) * float(BLOCK)
    share_ref[...] = weight * alive

    flags = jnp.concatenate((sums_ref[0], jnp.zeros((6, sums_ref.shape[2]), jnp.int32)), axis=0)
    flags = jnp.transpose(flags.astype(jnp.float32))
    for k in range(2):
        mask_ref[k] = jnp.broadcast_to(flags[:, k : k + 1], mask_ref.shape[1:])


def steer(t_ref, u_ref, fr_ref, fi_ref, lhs_ref, q):
    last = q == HALF // 2 - 1
    for h in range(2):
        cols = slice(128 * h, 128 * h + 128)
        for s in range(16):
            slab = slice(8 * s, 8 * s + 8)
            t, u = t_ref[slab, cols], u_ref[slab, cols]
            for i in range(2):
                m = HALF - 1 - 2 * q - i
                p, o = t * fr_ref[m, slab, cols], u * fi_ref[m, slab, cols]
                at = 16 * s + 8 * i
                lhs_ref[q, 0, at : at + 8, cols] = p - o
                at = 16 * s + 8 - 8 * i
                lhs_ref[q, 1, at : at + 8, cols] = p + o
            if last:
                fr, fi = fr_ref[HALF, slab, cols], fi_ref[HALF, slab, cols]
                t_ref[slab, cols] = t * fr + u * fi
                u_ref[slab, cols] = u * fr - t * fi


def multiply(g, channel, volt_ref, mask_ref, send_ref, keep_ref, lhs_ref, where_to, q):
    left = lax.broadcasted_iota(jnp.int32, (8, 128), 1) < 64
    sign = jnp.where(lax.broadcasted_iota(jnp.int32, (8, 128), 0) < 4, -1.0, 1.0)
    for side, pair in ((0, q), (1, HALF - 1 - q)):
        at = pl.multiple_of(g * (64 * GROUP) + pair * 128, 128)
        rhs = jnp.concatenate(
            (volt_ref[0, :, pl.ds(at, 128)], volt_ref[1, :, pl.ds(at, 128)]), axis=1
        )
        parts = []
        for h in range(2):
            keeps = [
                jnp.broadcast_to(mask_ref[h, pl.ds(channel + 2 * pair + i, 1), :], (8, 128))
                for i in range(2)
            ]
            keep = jnp.concatenate(keeps * 16, axis=0)
            value = lhs_ref[q, side, :, 128 * h : 128 * h + 128]
            parts.append(value.astype(jnp.bfloat16) * keep.astype(jnp.bfloat16))
        lhs = jnp.concatenate(parts, axis=1)
        both = jnp.dot(lhs, rhs, preferred_element_type=jnp.float32)
        for tile, (kept, place) in enumerate(where_to):
            one, two = both[16 * tile : 16 * tile + 8], both[16 * tile + 8 : 16 * tile + 16]
            by_real = jnp.where(left, one[:, :128], two[:, :128])
            by_imag = jnp.where(left, one[:, 128:], two[:, 128:])
            ref = keep_ref if kept else send_ref
            ref[8 * place : 8 * place + 8, pl.ds(at, 128)] = (
                by_real + pltpu.roll(by_imag, 4, 0) * sign
            )


def groups_of_chunk(
    first, count, final, volt_ref, t_ref, u_ref, fr_ref, fi_ref, mask_ref,
    send_ref, keep_ref, lhs_ref, where_to, wait,
):
    groups = count // GROUP
    quads = range(HALF // 2)
    tables = (t_ref, u_ref, fr_ref, fi_ref, lhs_ref)

    def part(g, q):
        multiply(
            g, first + g * GROUP, volt_ref, mask_ref, send_ref, keep_ref, lhs_ref, where_to, q
        )

    def group(g, carry):
        wait(g)
        for q in quads:
            part(g, q)
            steer(*tables, q)
        return carry

    lax.fori_loop(0, groups - 1 if final else groups, group, 0)
    if final:
        wait(groups - 1)
        for q in quads:
            part(groups - 1, q)


def put_counts(share_ref, first, count, send_ref, keep_ref, where_to):
    share = share_ref[...]
    share = pltpu.roll(share, (share.shape[1] - first) % share.shape[1], 1)[:, :PAD]
    for tile, (kept, place) in enumerate(where_to):
        ref = keep_ref if kept else send_ref
        ref[8 * place : 8 * place + 8, pl.ds(count * 64, PAD)] = share[8 * tile : 8 * tile + 8]


def loader(volt_hbm, volt_ref, sems, first, count):
    width = 64 * GROUP

    def piece(g):
        return pltpu.make_async_copy(
            volt_hbm.at[0, :, :, pl.ds(first * 64 + g * width, width)],
            volt_ref.at[:, :, pl.ds(g * width, width)],
            sems.at[g],
        )

    def load():
        for g in range(count // GROUP):
            piece(g).start()

    def ready(g=None):
        for i in range(count // GROUP) if g is None else (g,):
            piece(i).wait()

    return load, ready


def first_kernel(
    pos_hbm, dir_hbm, tap_hbm, index_hbm, flag_hbm, volt_hbm,
    send_ref, keep_ref, t_ref, u_ref, fr_ref, fi_ref, mask_ref, share_ref, lhs_ref, next_ref,
    pos_ref, dir_ref, tap_ref, index_ref, sums_ref, volt_ref,
    small_sems, sems, next_sems, *, chunk, spans, whole,
):
    first, count = spans[chunk]
    small = [
        pltpu.make_async_copy(src, dst, small_sems.at[i])
        for i, (src, dst) in enumerate((
            (pos_hbm, pos_ref), (dir_hbm, dir_ref), (tap_hbm, tap_ref),
            (index_hbm, index_ref), (flag_hbm, sums_ref),
        ))
    ]
    for copy in small:
        copy.start()
    load, ready = loader(volt_hbm, volt_ref, sems, first, count)
    load()
    ahead, arrived = loader(volt_hbm, next_ref, next_sems, *spans[chunk + 1])
    ahead()
    for copy in small:
        copy.wait()
    make_tables(
        pos_ref, dir_ref, tap_ref, index_ref,
        t_ref, u_ref, fr_ref, fi_ref, mask_ref, share_ref, sums_ref, whole,
    )
    where_to = places(CHUNKS[chunk][1])
    put_counts(share_ref, first, count, send_ref, keep_ref, where_to)

    for q in range(HALF // 2):
        steer(t_ref, u_ref, fr_ref, fi_ref, lhs_ref, q)
    groups_of_chunk(
        first, count, False, volt_ref, t_ref, u_ref, fr_ref, fi_ref, mask_ref,
        send_ref, keep_ref, lhs_ref, where_to, ready,
    )
    arrived()


def beam_later(
    volt_hbm, volt_ref, t_in, u_in, fr_ref, fi_ref, mask_ref, share_ref, lhs_in,
    send_ref, keep_ref, t_ref, u_ref, lhs_ref, next_ref, sems, *, chunk, spans,
):
    first, count = spans[chunk]
    last = chunk + 1 == len(spans)
    if not last:
        ahead, arrived = loader(volt_hbm, next_ref, sems, *spans[chunk + 1])
        ahead()
    where_to = places(CHUNKS[chunk][1])
    put_counts(share_ref, first, count, send_ref, keep_ref, where_to)
    groups_of_chunk(
        first, count, last, volt_ref, t_ref, u_ref, fr_ref, fi_ref, mask_ref,
        send_ref, keep_ref, lhs_ref, where_to, lambda g: None,
    )
    if not last:
        arrived()


def add_kernel(*refs, begin, rows):
    out_ref = refs[-1]
    total = None
    for ref in refs[:-1]:
        at = begin - (64 - ref.shape[0])
        part = ref[at : at + rows]
        total = part if total is None else total + part
    out_ref[...] = total


def power_kernel(*refs, first, count, more):
    power_ref, total_ref, buf, sem = refs[-4:]
    parts = refs[:5]
    left = lax.broadcasted_iota(jnp.int32, (8, 128), 1) < 64

    def summed(lanes):
        total = None
        for ref in parts:
            part = ref[ref.shape[0] - 8 :, lanes]
            total = part if total is None else total + part
        return total

    counts = summed(pl.ds(count * 64, PAD))
    whole = lax.broadcasted_iota(jnp.int32, (8, 128), 0) < 4
    whole = whole & (lax.broadcasted_iota(jnp.int32, (8, 128), 1) < count)
    inverse = 1.0 / jnp.where(whole, counts, 1.0)
    inverse = inverse * inverse
    total = refs[6][...] if more else jnp.zeros((8, 128), jnp.float32)
    for p in range(count // 2):
        value = summed(pl.ds(p * 128, 128))
        square = value * value
        square = square + pltpu.roll(square, 4, 0)
        scale = jnp.where(left, inverse[:, 2 * p : 2 * p + 1], inverse[:, 2 * p + 1 : 2 * p + 2])
        power = square * scale
        buf[:, pl.ds(p * 128, 128)] = power[:4]
        total = total + power
    copy = pltpu.make_async_copy(buf, power_ref.at[:, pl.ds(first * 64, count * 64)], sem.at[0])
    copy.start()
    if first + count == power_ref.shape[1] // 64:
        total = jnp.broadcast_to(jnp.sum(total, axis=1, keepdims=True), (8, 128))
    total_ref[...] = total
    copy.wait()


VMEM = pl.BlockSpec(memory_space=pltpu.VMEM)
HBM = pl.BlockSpec(memory_space=pltpu.HBM)


def limit(mib):
    return pltpu.CompilerParams(vmem_limit_bytes=mib * 2**20)


def on_device(voltages, positions, directions, flag_mask, tapers, weight_index):
    chan_local = flag_mask.shape[2]
    whole = chan_local * lax.axis_size("chan")
    spans = []
    for groups, _ in CHUNKS:
        spans.append((sum(s[1] for s in spans), groups * GROUP))

    def number(y, z, core):
        return (y * Z + z) * CORE + core

    def pairs(to):
        return [
            (number(y, z, c), number(*to(y, z, c)))
            for y in range(Y) for z in range(Z) for c in range(CORE)
        ]

    to_core = pairs(lambda y, z, c: (y, z, 1 - c))
    links = {
        "a": pairs(lambda y, z, c: (y, z ^ 1, c)),
        "b": pairs(lambda y, z, c: (y, z ^ 3, c)),
        "y": pairs(lambda y, z, c: (1 - y, z, c)),
    }

    def f32(*shape):
        return jax.ShapeDtypeStruct(shape, jnp.float32)

    def volts(chunk):
        return jax.ShapeDtypeStruct((2, 256, spans[chunk][1] * 64), jnp.bfloat16)

    def out(chunk):
        return f32(64, spans[chunk][1] * 64 + PAD)

    def in_hbm(x):
        return pltpu.with_memory_space_constraint(x, pltpu.HBM)

    voltages = in_hbm(voltages)
    steering = f32(HALF // 2, 2, 256, 256)
    table = f32(128, 256)
    factors = f32(HALF + 1, 128, 256)
    masks = f32(2, chan_local, 128)

    keeps, gots = [], []

    make = pl.pallas_call(
        lambda *refs: first_kernel(*refs, chunk=0, spans=spans, whole=whole),
        out_shape=(
            out(0), out(0), table, table, factors, factors, masks, f32(128, chan_local), steering,
            volts(1),
        ),
        in_specs=[HBM] * 6,
        out_specs=(VMEM,) * 10,
        scratch_shapes=[
            pltpu.VMEM((3, 1, 256), jnp.float32),
            pltpu.VMEM((3, 64), jnp.float32),
            pltpu.SMEM((1, 8), jnp.float32),
            pltpu.VMEM((1, 64), jnp.int32),
            pltpu.VMEM((1, 2, chan_local), jnp.int32),
            pltpu.VMEM(volts(0).shape, jnp.bfloat16),
            pltpu.SemaphoreType.DMA((5,)),
            pltpu.SemaphoreType.DMA((spans[0][1] // GROUP,)),
            pltpu.SemaphoreType.DMA((spans[1][1] // GROUP,)),
        ],
        compiler_params=limit(20),
        name="beam",
    )
    send, keep, t, u, fr, fi, mask, share, lhs, ahead = make(
        in_hbm(jnp.transpose(positions, (1, 0, 2))), in_hbm(directions), in_hbm(tapers),
        in_hbm(weight_index), in_hbm(flag_mask), voltages,
    )
    keeps.append(keep)
    gots.append([lax.ppermute(send, "stn", to_core)])

    def add(chunk, step):
        begin = (0, 32, 48)[step]
        rows = 32 >> step
        parts = [keeps[chunk], *gots[chunk]]
        lanes = out(chunk).shape[1]
        total = pl.pallas_call(
            lambda *refs: add_kernel(*refs, begin=begin, rows=rows),
            out_shape=f32(rows, lanes),
            in_specs=[VMEM] * len(parts),
            out_specs=VMEM,
            compiler_params=limit(8),
            name="add",
        )(*parts)
        to = links[CHUNKS[chunk][1][step]]
        gots[chunk].append(lax.ppermute(total, "stn", to))

    for chunk in range(1, len(spans)):
        last = chunk + 1 == len(spans)
        nexts = f32(8, 128) if last else volts(chunk + 1)
        count = 1 if last else spans[chunk + 1][1] // GROUP
        send, keep, t, u, lhs, ahead = pl.pallas_call(
            lambda *refs, chunk=chunk: beam_later(*refs, chunk=chunk, spans=spans),
            out_shape=(out(chunk), out(chunk), table, table, steering, nexts),
            in_specs=[HBM] + [VMEM] * 8,
            out_specs=(VMEM,) * 6,
            input_output_aliases={2: 2, 3: 3, 8: 4},
            scratch_shapes=[pltpu.SemaphoreType.DMA((count,))],
            compiler_params=limit(8),
            name="beam",
        )(voltages, ahead, t, u, fr, fi, mask, share, lhs)
        keeps.append(keep)
        gots.append([lax.ppermute(send, "stn", to_core)])
    for step in range(3):
        for chunk in range(len(spans)):
            add(chunk, step)

    power = total = None
    for chunk, (first, count) in enumerate(spans):
        more = chunk > 0
        extra = [power, total] if more else []
        power, total = pl.pallas_call(
            lambda *refs, first=first, count=count, more=more: power_kernel(
                *refs, first=first, count=count, more=more
            ),
            out_shape=(f32(4, chan_local * 64), f32(8, 128)),
            in_specs=[VMEM] * 5 + ([HBM, VMEM] if more else []),
            out_specs=(HBM, VMEM),
            scratch_shapes=[
                pltpu.VMEM((4, count * 64), jnp.float32), pltpu.SemaphoreType.DMA((1,))
            ],
            input_output_aliases={5: 0} if more else {},
            compiler_params=limit(8),
            name="power",
        )(keeps[chunk], *gots[chunk], *extra)
    n = lax.axis_size("chan")
    for flip in (1, 3, 4):
        total = total + lax.ppermute(total, "chan", [(i, i ^ flip) for i in range(n)])
    return (power, total[:4, 0])


def solution(mesh):
    in_specs = (
        P("stn", None, None, "chan"),
        P("stn", None, None),
        P(),
        P("stn", None, "chan"),
        P("stn", None),
        P("stn", None),
    )
    out_specs = (P("stn", "chan"), P("stn"))
    return jax.shard_map(
        on_device, mesh=mesh, in_specs=in_specs, out_specs=out_specs, check_vma=False
    )
```

```python
import jax
import jax.numpy as jnp
from jax import lax
from jax.experimental import pallas as pl
from jax.experimental.pallas import tpu as pltpu
from jax.sharding import PartitionSpec as P


BLOCK = 128
GROUP = 16
HALF = GROUP // 2
TABLE_ROWS = 136
Y, Z, CORE = 2, 4, 2
CHUNKS = ((4, "yab"), (4, "bya"), (4, "aby"), (2, "yba"), (2, "bay"))
COUNTS = 1
FINISH = (1, 0, 2, 4, 3)

SIN = (
    6.283185307136744,
    -41.34170221839102,
    81.60524742222256,
    -76.70580022497265,
    42.057754062457725,
    -15.086565424172946,
    3.781319130391277,
    -0.6207787856421599,
)
COS = (
    0.9999999998857545,
    -19.73920874347965,
    64.93938907682282,
    -85.4566583290415,
    60.24213144377024,
    -26.404668561864113,
    7.800131962320425,
    -1.4531123696403512,
)
SIN_NEAR = (6.283185307179586, -41.34170224039975, 81.60524927607504)
COS_NEAR = (1.0, -19.739208802178716, 64.93939402266829, -85.45681720669373)


def poly(coefs, x):
    total = jnp.full(x.shape, coefs[-1], jnp.float32)
    for c in coefs[-2::-1]:
        total = total * x + c
    return total


def places(order):
    out = []
    for tile in range(16):
        moved = {"y": (tile // 4) % 2, "b": (tile // 2) % 2, "a": tile % 2}
        at = sum((1 - moved[name]) << (2 - i) for i, name in enumerate(order))
        out.append((tile // 8, at))
    return out


def make_tables(
    pos_ref, dir_ref, tap_ref, index_ref, sums_ref, table_ref, mask_ref, whole,
):
    me = lax.axis_index("stn")
    my_core = me % CORE
    my_z = (me // CORE) % Z
    my_y = me // (CORE * Z)
    rows = lax.broadcasted_iota(jnp.int32, (128, 64), 0)
    tile, sub = rows // 8, rows % 8
    core = jnp.where(tile // 8 == 1, my_core, 1 - my_core)
    y = jnp.bitwise_xor((tile // 4) % 2, my_y)
    z = jnp.bitwise_xor(jnp.bitwise_xor(tile % 2, 3 * ((tile // 2) % 2)), my_z)
    beam = y * (64 // Y) + z * (64 // (Y * Z)) + core * 4 + sub % 4
    chosen = beam == lax.broadcasted_iota(jnp.int32, (128, 64), 1)

    def column(row):
        return jnp.sum(jnp.where(chosen, row, 0.0), axis=1, keepdims=True)

    weight_row = jnp.zeros((1, 64), jnp.float32)
    for e in range(tap_ref.shape[1]):
        weight_row = weight_row + jnp.where(index_ref[...] == e, tap_ref[0, e], 0.0)
    weight = column(weight_row)
    delay = (
        column(dir_ref[0:1, :]) * pos_ref[0]
        + column(dir_ref[1:2, :]) * pos_ref[1]
        + column(dir_ref[2:3, :]) * pos_ref[2]
    )
    channel = lax.axis_index("chan") * (whole // lax.axis_size("chan"))
    ratio = 1.0 + 0.5 * ((channel.astype(jnp.float32) + (HALF - 0.5)) / whole)
    turns = delay * ratio
    r = turns - jnp.round(turns)
    x = r * r
    cos, sin = poly(COS, x), r * poly(SIN, x)
    real = lax.broadcasted_iota(jnp.int32, (128, 256), 0) % 8 < 4
    table_ref[0, 0:128] = weight * jnp.where(real, cos, -sin)
    table_ref[1, 0:128] = weight * jnp.where(real, sin, cos)
    step = delay * (0.5 / whole)

    def factor(r):
        x = r * r
        return poly(COS_NEAR, x), -(r * poly(SIN_NEAR, x))

    def times(v, w):
        return v[0] * w[0] - v[1] * w[1], v[0] * w[1] + v[1] * w[0]

    half = factor(0.5 * step)
    one = factor(step)
    for j in range(HALF):
        table_ref[2 + 2 * j, 0:128], table_ref[3 + 2 * j, 0:128] = half
        last, half = half, times(half, one)
    last = times(half, last)
    table_ref[2 + 2 * HALF, 0:128], table_ref[3 + 2 * HALF, 0:128] = last
    alive = (sums_ref[0, 0:1, :] + sums_ref[0, 1:2, :]).astype(jnp.float32) * float(BLOCK)

    flags = jnp.concatenate((sums_ref[0], jnp.zeros((6, sums_ref.shape[2]), jnp.int32)), axis=0)
    flags = jnp.transpose(flags.astype(jnp.float32))
    for k in range(2):
        mask_ref[k] = jnp.broadcast_to(flags[:, k : k + 1], mask_ref.shape[1:])
    return weight * alive


def steer(table_ref, lhs_ref, q):
    last = q == HALF // 2 - 1
    for h in range(2):
        cols = slice(128 * h, 128 * h + 128)
        for s in range(16):
            slab = slice(8 * s, 8 * s + 8)
            t, u = table_ref[0, slab, cols], table_ref[1, slab, cols]
            for i in range(2):
                m = HALF - 1 - 2 * q - i
                p = t * table_ref[2 + 2 * m, slab, cols]
                o = u * table_ref[3 + 2 * m, slab, cols]
                at = 16 * s + 8 * i
                lhs_ref[q, 0, at : at + 8, cols] = p - o
                at = 16 * s + 8 - 8 * i
                lhs_ref[q, 1, at : at + 8, cols] = p + o
            if last:
                fr, fi = table_ref[2 + 2 * HALF, slab, cols], table_ref[3 + 2 * HALF, slab, cols]
                table_ref[0, slab, cols] = t * fr + u * fi
                table_ref[1, slab, cols] = u * fr - t * fi


def multiply(g, channel, volt_ref, mask_ref, send_ref, keep_ref, lhs_ref, where_to, q):
    left = lax.broadcasted_iota(jnp.int32, (8, 128), 1) < 64
    sign = jnp.where(lax.broadcasted_iota(jnp.int32, (8, 128), 0) < 4, -1.0, 1.0)
    for side, pair in ((0, q), (1, HALF - 1 - q)):
        at = pl.multiple_of(g * (64 * GROUP) + pair * 128, 128)
        rhs = jnp.concatenate(
            (volt_ref[0, :, pl.ds(at, 128)], volt_ref[1, :, pl.ds(at, 128)]), axis=1
        )
        parts = []
        for h in range(2):
            keeps = [
                jnp.broadcast_to(mask_ref[h, pl.ds(channel + 2 * pair + i, 1), :], (8, 128))
                for i in range(2)
            ]
            keep = jnp.concatenate(keeps * 16, axis=0)
            value = lhs_ref[q, side, 0:256, 128 * h : 128 * h + 128]
            parts.append(value.astype(jnp.bfloat16) * keep.astype(jnp.bfloat16))
        lhs = jnp.concatenate(parts, axis=1)
        both = jnp.dot(lhs, rhs, preferred_element_type=jnp.float32)
        for tile, (kept, place) in enumerate(where_to):
            one, two = both[16 * tile : 16 * tile + 8], both[16 * tile + 8 : 16 * tile + 16]
            by_real = jnp.where(left, one[:, :128], two[:, :128])
            by_imag = jnp.where(left, one[:, 128:], two[:, 128:])
            ref = keep_ref if kept else send_ref
            ref[8 * place : 8 * place + 8, pl.ds(at, 128)] = (
                by_real + pltpu.roll(by_imag, 4, 0) * sign
            )


def groups_of_chunk(
    first, count, final, volt_ref, table_ref, mask_ref, send_ref, keep_ref, lhs_ref,
    where_to, wait,
):
    groups = count // GROUP
    steered = groups - 1 if final else groups

    def one(g, steering=True):
        for q in range(HALF // 2):
            multiply(
                g, first + g * GROUP, volt_ref, mask_ref, send_ref, keep_ref, lhs_ref, where_to, q
            )
            if steering:
                steer(table_ref, lhs_ref, q)

    def two(i, carry):
        wait(2 * i, 2)
        one(2 * i)
        one(2 * i + 1)
        return carry

    if steered // 2 > 1:
        lax.fori_loop(0, steered // 2, two, 0)
    elif steered // 2:
        two(0, 0)
    if steered % 2:
        wait(steered - 1, 1)
        one(steered - 1)
    if final:
        one(groups - 1, False)


def loader(volt_hbm, volt_ref, sems, first, count):
    width = 64 * GROUP

    def piece(g):
        return pltpu.make_async_copy(
            volt_hbm.at[0, :, :, pl.ds(first * 64 + g * width, width)],
            volt_ref.at[:, :, pl.ds(g * width, width)],
            sems.at[g],
        )

    def load(begin=0, end=count // GROUP):
        for g in range(begin, end):
            piece(g).start()

    def ready(g=None):
        for i in range(count // GROUP) if g is None else (g,):
            piece(i).wait()

    return load, ready


def put_counts(share_ref, chunk, count, send_ref, keep_ref):
    if chunk != COUNTS:
        return
    for tile, (kept, place) in enumerate(places(CHUNKS[chunk][1])):
        ref = keep_ref if kept else send_ref
        ref[8 * place : 8 * place + 8, pl.ds(count * 64, share_ref.shape[1])] = (
            share_ref[8 * tile : 8 * tile + 8]
        )


def first_kernel(
    pos_hbm, dir_hbm, tap_hbm, index_hbm, flag_hbm, volt_hbm,
    send_ref, keep_ref, table_ref, mask_ref, share_ref, lhs_ref, next_ref,
    pos_ref, dir_ref, tap_ref, index_ref, sums_ref, volt_ref,
    small_sems, sems, next_sems, *, spans, whole,
):
    first, count = spans[0]
    small = [
        pltpu.make_async_copy(src, dst, small_sems.at[i])
        for i, (src, dst) in enumerate((
            (pos_hbm, pos_ref), (dir_hbm, dir_ref), (tap_hbm, tap_ref),
            (index_hbm, index_ref), (flag_hbm, sums_ref),
        ))
    ]
    for copy in small:
        copy.start()
    load, ready = loader(volt_hbm, volt_ref, sems, first, count)
    early = min(2, count // GROUP)
    load(0, early)
    ahead, arrived = loader(volt_hbm, next_ref, next_sems, *spans[1])
    for copy in small:
        copy.wait()
    share = make_tables(
        pos_ref, dir_ref, tap_ref, index_ref, sums_ref, table_ref, mask_ref, whole
    )
    share_ref[...] = share
    put_counts(share_ref, 0, count, send_ref, keep_ref)
    for q in range(HALF // 2):
        steer(table_ref, lhs_ref, q)
    for g in range(early):
        ready(g)
    load(early)
    ahead()

    def wait(g, n):
        def arrive():
            for i in range(n):
                ready(g + i)

        if isinstance(g, int):
            if g >= early:
                arrive()
        else:
            pl.when(g > 0)(arrive)

    groups_of_chunk(
        first, count, False, volt_ref, table_ref, mask_ref, send_ref, keep_ref, lhs_ref,
        places(CHUNKS[0][1]), wait,
    )
    arrived()


def beam_later(
    volt_hbm, volt_ref, mask_ref, share_ref, table_in, lhs_in,
    send_ref, keep_ref, table_ref, lhs_ref, next_ref, sems, *, chunk, spans,
):
    first, count = spans[chunk]
    last = chunk + 1 == len(spans)
    if not last:
        ahead, arrived = loader(volt_hbm, next_ref, sems, *spans[chunk + 1])
        ahead()
    put_counts(share_ref, chunk, count, send_ref, keep_ref)
    where_to = places(CHUNKS[chunk][1])
    groups_of_chunk(
        first, count, last, volt_ref, table_ref, mask_ref, send_ref, keep_ref, lhs_ref,
        where_to, lambda g, n: None,
    )
    if not last:
        arrived()


def add_kernel(*refs, begin, rows):
    out_ref = refs[-1]
    total = None
    for ref in refs[:-1]:
        at = begin - (64 - ref.shape[0])
        part = ref[at : at + rows]
        total = part if total is None else total + part
    out_ref[...] = total


def power_kernel(*refs, first, count, counts_here, final):
    parts = refs[:5]
    left = lax.broadcasted_iota(jnp.int32, (8, 128), 1) < 64

    def summed(lanes):
        total = None
        for ref in parts:
            part = ref[ref.shape[0] - 8 :, lanes]
            total = part if total is None else total + part
        return total

    if counts_here:
        power_ref, total_ref, inverse_ref = refs[5:]
        counts = summed(pl.ds(count * 64, inverse_ref.shape[1]))
        used = lax.broadcasted_iota(jnp.int32, counts.shape, 0) < 4
        inverse = 1.0 / jnp.where(used, counts, 1.0)
        inverse_ref[...] = inverse * inverse
        total = jnp.zeros((8, 128), jnp.float32)
    else:
        total_in, inverse_ref, power_ref, total_ref = refs[5:]
        total = total_in[...]
    for p in range(count // 2):
        value = summed(pl.ds(p * 128, 128))
        square = value * value
        square = square + pltpu.roll(square, 4, 0)
        c = first + 2 * p
        scale = jnp.where(left, inverse_ref[:, c : c + 1], inverse_ref[:, c + 1 : c + 2])
        power = square * scale
        power_ref[:, pl.ds(p * 128, 128)] = power
        total = total + power
    if final:
        total = jnp.broadcast_to(jnp.sum(total, axis=1, keepdims=True), (8, 128))
    total_ref[...] = total


def store_kernel(*refs, spans):
    power_hbm, buf, sem = refs[-3:]
    for ref, (first, count) in zip(refs, spans):
        buf[:, pl.ds(first * 64, count * 64)] = ref[0:4]
    copy = pltpu.make_async_copy(buf, power_hbm, sem.at[0])
    copy.start()
    copy.wait()


VMEM = pl.BlockSpec(memory_space=pltpu.VMEM)
HBM = pl.BlockSpec(memory_space=pltpu.HBM)


def limit(mib):
    return pltpu.CompilerParams(vmem_limit_bytes=mib * 2**20)


def on_device(voltages, positions, directions, flag_mask, tapers, weight_index):
    chan_local = flag_mask.shape[2]
    whole = chan_local * lax.axis_size("chan")
    spans = []
    for groups, _ in CHUNKS:
        spans.append((sum(s[1] for s in spans), groups * GROUP))

    def number(y, z, core):
        return (y * Z + z) * CORE + core

    def pairs(to):
        return [
            (number(y, z, c), number(*to(y, z, c)))
            for y in range(Y) for z in range(Z) for c in range(CORE)
        ]

    to_core = pairs(lambda y, z, c: (y, z, 1 - c))
    links = {
        "a": pairs(lambda y, z, c: (y, z ^ 1, c)),
        "b": pairs(lambda y, z, c: (y, z ^ 3, c)),
        "y": pairs(lambda y, z, c: (1 - y, z, c)),
    }

    def f32(*shape):
        return jax.ShapeDtypeStruct(shape, jnp.float32)

    def volts(chunk):
        return jax.ShapeDtypeStruct((2, 256, spans[chunk][1] * 64), jnp.bfloat16)

    def out(chunk):
        return f32(64, spans[chunk][1] * 64 + (chan_local if chunk == COUNTS else 0))

    def in_hbm(x):
        return pltpu.with_memory_space_constraint(x, pltpu.HBM)

    voltages = in_hbm(voltages)
    table = f32(2 * HALF + 4, TABLE_ROWS, 256)
    steering = f32(HALF // 2, 2, 264, 256)
    masks = f32(2, chan_local, 128)
    shares = f32(128, chan_local)
    keeps, gots = [], []

    make = pl.pallas_call(
        lambda *refs: first_kernel(*refs, spans=spans, whole=whole),
        out_shape=(out(0), out(0), table, masks, shares, steering, volts(1)),
        in_specs=[HBM] * 6,
        out_specs=(VMEM,) * 7,
        scratch_shapes=[
            pltpu.VMEM((3, 1, 256), jnp.float32),
            pltpu.VMEM((3, 64), jnp.float32),
            pltpu.SMEM((1, 8), jnp.float32),
            pltpu.VMEM((1, 64), jnp.int32),
            pltpu.VMEM((1, 2, chan_local), jnp.int32),
            pltpu.VMEM(volts(0).shape, jnp.bfloat16),
            pltpu.SemaphoreType.DMA((5,)),
            pltpu.SemaphoreType.DMA((spans[0][1] // GROUP,)),
            pltpu.SemaphoreType.DMA((spans[1][1] // GROUP,)),
        ],
        compiler_params=limit(20),
        name="beam",
    )
    send, keep, table_now, mask, share, lhs, ahead = make(
        in_hbm(jnp.transpose(positions, (1, 0, 2))), in_hbm(directions), in_hbm(tapers),
        in_hbm(weight_index), in_hbm(flag_mask), voltages,
    )
    keeps.append(keep)
    gots.append([lax.ppermute(send, "stn", to_core)])

    def add(chunk, step):
        begin = (0, 32, 48)[step]
        rows = 32 >> step
        parts = [keeps[chunk], *gots[chunk]]
        lanes = out(chunk).shape[1]
        total = pl.pallas_call(
            lambda *refs: add_kernel(*refs, begin=begin, rows=rows),
            out_shape=f32(rows, lanes),
            in_specs=[VMEM] * len(parts),
            out_specs=VMEM,
            compiler_params=limit(8),
            name="add",
        )(*parts)
        to = links[CHUNKS[chunk][1][step]]
        gots[chunk].append(lax.ppermute(total, "stn", to))

    for chunk in range(1, len(spans)):
        last = chunk + 1 == len(spans)
        nexts = f32(8, 128) if last else volts(chunk + 1)
        count = 1 if last else spans[chunk + 1][1] // GROUP
        send, keep, table_now, lhs, ahead = pl.pallas_call(
            lambda *refs, chunk=chunk: beam_later(*refs, chunk=chunk, spans=spans),
            out_shape=(out(chunk), out(chunk), table, steering, nexts),
            in_specs=[HBM] + [VMEM] * 5,
            out_specs=(VMEM,) * 5,
            input_output_aliases={4: 2, 5: 3},
            scratch_shapes=[pltpu.SemaphoreType.DMA((count,))],
            compiler_params=limit(8),
            name="beam",
        )(voltages, ahead, mask, share, table_now, lhs)
        keeps.append(keep)
        gots.append([lax.ppermute(send, "stn", to_core)])
    for step in range(3):
        for chunk in range(len(spans)):
            add(chunk, step)

    powers, extra = {}, []
    for chunk in FINISH:
        first, count = spans[chunk]
        here, final = chunk == COUNTS, chunk == FINISH[-1]
        shapes = (f32(8, count * 64), f32(8, 128)) + ((f32(8, chan_local),) if here else ())
        power, total, *inverse = pl.pallas_call(
            lambda *refs, first=first, count=count, here=here, final=final: power_kernel(
                *refs, first=first, count=count, counts_here=here, final=final
            ),
            out_shape=shapes,
            in_specs=[VMEM] * (5 + len(extra)),
            out_specs=(VMEM,) * len(shapes),
            compiler_params=limit(4),
            name="power",
        )(keeps[chunk], *gots[chunk], *extra)
        powers[chunk] = power
        extra = [total, inverse[0] if inverse else extra[1]]

    n = lax.axis_size("chan")

    def other(flip):
        return lax.ppermute(total, "chan", [(i, i ^ flip) for i in range(n)])

    far = [other(flip) for flip in (3, 2, 1)]
    total = (total + far[2]) + (far[1] + far[0])
    total = total + other(4)
    power = pl.pallas_call(
        lambda *refs: store_kernel(*refs, spans=spans),
        out_shape=f32(4, chan_local * 64),
        in_specs=[VMEM] * len(spans),
        out_specs=HBM,
        scratch_shapes=[
            pltpu.VMEM((4, chan_local * 64), jnp.float32), pltpu.SemaphoreType.DMA((1,))
        ],
        compiler_params=limit(4),
        name="store",
    )(*[powers[chunk] for chunk in range(len(spans))])
    return (power, total[:4, 0])


def solution(mesh):
    in_specs = (
        P("stn", None, None, "chan"),
        P("stn", None, None),
        P(),
        P("stn", None, "chan"),
        P("stn", None),
        P("stn", None),
    )
    out_specs = (P("stn", "chan"), P("stn"))
    return jax.shard_map(
        on_device, mesh=mesh, in_specs=in_specs, out_specs=out_specs, check_vma=False
    )
```
